32 devices in a mesh: replica: 2 (over x), pipe: 4 (over z), tensor: 4 (over y, core).
Axes of the slice: x: 2, y: 2, z: 4, core: 2. Of those that a mesh axis runs over, the one named last changes fastest.
Arguments:
- queries: bfloat16 [256, 8192], P('replica', ('pipe', 'tensor')), parts along dimension 0, may hold values from -128 to 128, as said below
- cache_keys: bfloat16 [8, 4096, 1024], P('replica', 'tensor', 'pipe'), parts along dimension 0, may hold values from -4 to 4
- cache_values: bfloat16 [8, 4096, 1024], P('replica', 'tensor', 'pipe'), parts along dimension 0, may hold values from -6 to 6
- prefix_lengths: int32 [8], P('replica'), parts along dimension 0, may hold values from 2048 to 4064
- residual_in: bfloat16 [256, 8192], P('replica', ('pipe', 'tensor')), parts along dimension 0, may hold values from -64 to 64
- out_weight: bfloat16 [8192, 4, 2048], P('pipe', None, 'tensor'), may hold values from -0.0625 to 0.0625
- norm_gain: float32 [8192], P(('pipe', 'tensor')), may hold values from 0.1 to 1.9
Outputs:
- residual_out: bfloat16 [256, 8192], P('replica', ('pipe', 'tensor')), parts along dimension 0
- normed: bfloat16 [256, 8192], P('replica', ('pipe', 'tensor')), parts along dimension 0
The draws below stay inside these ranges and needn't reach their ends.
There are 2 independent parts, one for each index of `replica`. The reference program is written for one: setup_inputs(seed, part) draws one part's arguments, and reference() takes and returns one part's arrays. A program takes and returns all parts, laid end to end along the dimension named above; an argument that names none is the same for every part. Nothing has to cross between parts.
Inputs may be any that keep to these rules, and one draw needn't show every extreme that they name: `queries`: entries of the query rows; some rows may be much longer than others. The span's own keys and values already stand in the cache, in slots prefix_lengths[r] to prefix_lengths[r] + 31; later slots hold unused entries.
All inputs are finite; a program needn't handle non-finite values.
Results may differ from the reference program's by a relative error of at most 0.018.
Values may be sent and summed in bfloat16 or wider, within the bound.
A program may use at most 64 MiB of HBM per device.

```python
import math
import jax
import jax.numpy as jnp
from jax import lax

D = 8192
HEADS = 64
KV_HEADS = 8
HD = 128
C = 32
L = 4096
R = 4
N_PIPE = 4


def draw_queries(key, part):
    drawn = 2.5 * jnp.clip(jax.random.normal(jax.random.fold_in(key, 1), (R, C, HEADS, HD), jnp.float32), -6.0, 6.0)
    return drawn.reshape(R * C, HEADS * HD).astype(jnp.bfloat16)


def draw_cache_keys(key, part):
    drawn = jnp.clip(jax.random.normal(jax.random.fold_in(key, 2), (R, L, KV_HEADS, HD), jnp.float32), -4.0, 4.0)
    return drawn.reshape(R, L, KV_HEADS * HD).astype(jnp.bfloat16)


def draw_residual_in(key, part):
    row_scale = 0.03 * jnp.exp(jax.random.uniform(jax.random.fold_in(key, 3), (R * C, 1), jnp.float32, 0.0, math.log(10.0)))
    column_trend = jnp.sqrt(1.0 + 2.0 * jnp.arange(D, dtype=jnp.float32) / max(D - 1, 1))[None, :]
    column_scale = jnp.exp(jax.random.uniform(jax.random.fold_in(key, 4), (1, D), jnp.float32, 0.0, math.log(10.0))) * column_trend
    noise = jnp.clip(jax.random.normal(jax.random.fold_in(key, 6), (R * C, D), jnp.float32), -4.0, 4.0)
    drawn = noise * row_scale * column_scale
    return drawn.astype(jnp.bfloat16)


def touch_ends(entries, own_key, low, high):
    place = [jax.random.randint(jax.random.fold_in(own_key, axis), (), 0, length) for axis, length in enumerate(entries.shape)]
    widest = entries.shape.index(max(entries.shape))
    neighbour = place[:widest] + [(place[widest] + 1) % entries.shape[widest]] + place[widest + 1:]
    return entries.at[tuple(place)].set(low).at[tuple(neighbour)].set(high)


def steps_of(stream_key, dims, split, low, top_value):
    level, own = 1.0, jax.random.fold_in(stream_key, 6)
    for axis_at, blocks in split:
        steps = jnp.exp(jax.random.uniform(jax.random.fold_in(own, axis_at), (blocks,), jnp.float32, low / len(split), top_value / len(split)))
        level = level * jnp.repeat(steps, dims[axis_at] // blocks).reshape([-1 if axis == axis_at else 1 for axis in range(len(dims))])
    return level


def centred(own_key, extent, deviation, most, shards=(), kind=jnp.bfloat16):
    values = deviation * jax.random.normal(own_key, extent, jnp.float32)
    if shards:
        values = values * steps_of(own_key, extent, shards, -0.22, 0.18)
    return jnp.clip(values, -most, most).astype(kind)


def setup_inputs(seed: int = 0, part: int = 0) -> dict:
    streams_of = jax.random.split(jax.random.key(seed), 8)
    part_splits = jax.random.split(jax.random.fold_in(streams_of[7], part), 8)
    return {
        "queries": draw_queries(jax.random.fold_in(jax.random.fold_in(streams_of[7], part), 71), part),
        "cache_keys": draw_cache_keys(jax.random.fold_in(jax.random.fold_in(streams_of[7], part), 71), part),
        "cache_values": centred(part_splits[2], (R, L, KV_HEADS * HD), 1.0, 6.0, ((1, 4), (2, 4))),
        "prefix_lengths": touch_ends(jax.random.randint(part_splits[3], (R,), L // 2, L - C + 1), jax.random.fold_in(part_splits[3], 1), L // 2, L - C).astype(jnp.int32),
        "residual_in": draw_residual_in(jax.random.fold_in(jax.random.fold_in(streams_of[7], part), 71), part),
        "out_weight": centred(streams_of[5], (HEADS * HD, N_PIPE, D // N_PIPE), (HEADS * HD) ** -0.5, 0.0625, ((0, 4), (2, 4))),
        "norm_gain": jnp.clip(1.0 + 0.18 * jax.random.normal(streams_of[6], (D,), jnp.float32), 0.1, 1.9),
    }


masked_value = -1e+30
epsilon = 1e-05

def attend_request(packed):
    request_queries, request_keys, request_values, prefix = packed
    group_size = HEADS // KV_HEADS
    queries_here = request_queries.reshape(C, KV_HEADS, group_size, HD).astype(jnp.float32)
    keys_here = request_keys.reshape(L, KV_HEADS, HD).astype(jnp.float32)
    values_here = request_values.reshape(L, KV_HEADS, HD).astype(jnp.float32)
    scores = jnp.einsum('cghd,jgd->cghj', queries_here, keys_here) * (1.0 / math.sqrt(HD))
    limits = prefix + jnp.arange(C, dtype=jnp.int32)
    visible = jnp.arange(L, dtype=jnp.int32)[None, :] <= limits[:, None]
    visible = visible[:, None, None, :]
    masked = jnp.where(visible, scores, masked_value)
    row_peak = lax.optimization_barrier(jnp.max(masked, axis=-1, keepdims=True))
    weights = jnp.where(visible, jnp.exp(masked - row_peak), 0.0)
    row_total = lax.optimization_barrier(jnp.sum(weights, axis=-1))
    rounded = lax.optimization_barrier(weights.astype(jnp.bfloat16)).astype(jnp.float32)
    summed = jnp.einsum('cghj,jgd->cghd', rounded, values_here)
    return (summed / row_total[..., None]).astype(jnp.bfloat16)

def reference(queries, cache_keys, cache_values, prefix_lengths, residual_in, out_weight, norm_gain):
    per_request = queries.reshape(R, C, HEADS * HD)
    attended = lax.map(attend_request, (per_request, cache_keys, cache_values, prefix_lengths))
    attended = attended.reshape(R * C, HEADS * HD)
    weight_matrix = out_weight.reshape(HEADS * HD, D)
    section_rows = HEADS * HD // N_PIPE
    projected = jnp.zeros((R * C, D), jnp.float32)
    for section_index in range(N_PIPE):
        lower = section_index * section_rows
        section_term = jnp.dot(attended[:, lower:lower + section_rows], weight_matrix[lower:lower + section_rows], preferred_element_type=jnp.float32)
        projected = projected + lax.optimization_barrier(section_term.astype(jnp.bfloat16)).astype(jnp.float32)
    updated = residual_in.astype(jnp.float32) + projected
    squares = lax.optimization_barrier(jnp.sum(updated * updated, axis=1, keepdims=True))
    normed = updated * lax.rsqrt(squares / D + epsilon) * norm_gain.astype(jnp.float32)[None, :]
    return (updated.astype(jnp.bfloat16), normed.astype(jnp.bfloat16))
```

```python
import functools
import math

import jax
import jax.numpy as jnp
from jax import lax
from jax.experimental import pallas as pl
from jax.experimental.pallas import tpu as pltpu
from jax.sharding import PartitionSpec as P

HD = 128
LANES = 128
masked_value = -1e30
lowest_peak = -1e29
epsilon = 1e-05
MESH = pl.DeviceIdType.MESH


def kernel(
    n_pipe,
    n_tensor,
    requests,
    prefix_ref,
    q_hbm,
    k_hbm,
    v_hbm,
    w_hbm,
    res_ref,
    gain_ref,
    residual_out,
    normed_out,
    q_all,
    keys,
    values,
    w_raw,
    w_ready,
    o_send,
    st_send,
    o_recv,
    st_recv,
    att,
    acc,
    p_send,
    p_recv,
    sq_send,
    sq_recv,
    q_local_sem,
    kv_sem,
    w_sem,
    q_send_sem,
    q_recv_sem,
    o_sems,
    st_sems,
    att_send_sem,
    att_recv_sem,
    p_sems,
    sq_sems,
):
    tokens = res_ref.shape[0]
    span = tokens // requests
    heads = q_hbm.shape[1] // HD
    rows = heads * span
    chips = n_tensor // 2
    n_groups, slots = keys.shape[1], keys.shape[2]
    group_size = n_tensor * heads // n_groups
    col_groups, depth, width = w_ready.shape
    depth_each = depth // n_tensor
    devices = n_pipe * n_tensor
    coef = math.log2(math.e) / math.sqrt(HD)

    me_p = lax.axis_index("pipe")
    me = lax.axis_index("tensor")
    chip = me // 2
    core = lax.rem(me, 2)
    partner = chip * 2 + 1 - core
    flat = me_p * n_tensor + me

    def other_chip(d):
        return lax.rem(chip + d, chips)

    def group_of(c):
        return (c * 2 * heads) // group_size

    def q_local(r, h):
        return pltpu.make_async_copy(
            q_hbm.at[pl.ds(r * span, span), pl.ds(h * HD, HD)],
            q_all.at[chip, r, pl.ds(core * rows + h * span, span)],
            q_local_sem.at[r, h],
        )

    def kv_copy(which, r, g):
        src, dst = ((k_hbm, keys), (v_hbm, values))[which]
        return pltpu.make_async_copy(
            src.at[r, :, pl.ds(pl.multiple_of(g * HD, HD), HD)], dst.at[r, g], kv_sem.at[which, r, g]
        )

    for r in range(requests):
        for h in range(heads):
            q_local(r, h).start()
    for gi in range(n_groups):
        for r in range(requests):
            g = lax.rem(group_of(chip) + gi, n_groups)
            kv_copy(0, r, g).start()
            kv_copy(1, r, g).start()
    w_copy = pltpu.make_async_copy(w_hbm, w_raw, w_sem)
    w_copy.start()

    barrier = pltpu.get_barrier_semaphore()

    def greet(i, carry):
        other = lax.rem(flat + i, devices)
        pl.semaphore_signal(
            barrier,
            inc=1,
            device_id={"pipe": other // n_tensor, "tensor": lax.rem(other, n_tensor)},
            device_id_type=MESH,
        )
        return carry

    lax.fori_loop(1, devices, greet, 0)
    pl.semaphore_wait(barrier, devices - 1)

    def q_piece(owner_chip, owner_core, r, hop, target):
        piece = q_all.at[owner_chip, r, pl.ds(owner_core * rows, rows)]
        return pltpu.make_async_remote_copy(
            src_ref=piece,
            dst_ref=piece,
            send_sem=q_send_sem.at[hop, r],
            recv_sem=q_recv_sem.at[owner_chip * 2 + owner_core, r],
            device_id={"tensor": target},
            device_id_type=MESH,
        )

    for r in range(requests):
        for h in range(heads):
            q_local(r, h).wait()
        for d in range(1, chips):
            q_piece(chip, core, r, d, other_chip(d) * 2 + core).start()
        q_piece(chip, core, r, 0, partner).start()

    def parts_to(target, r):
        return (
            pltpu.make_async_remote_copy(
                src_ref=o_send.at[target, r],
                dst_ref=o_recv.at[me, r],
                send_sem=o_sems.at[0, target, r],
                recv_sem=o_sems.at[1, me, r],
                device_id={"tensor": target},
                device_id_type=MESH,
            ),
            pltpu.make_async_remote_copy(
                src_ref=st_send.at[target, r],
                dst_ref=st_recv.at[me, r],
                send_sem=st_sems.at[0, target, r],
                recv_sem=st_sems.at[1, me, r],
                device_id={"tensor": target},
                device_id_type=MESH,
            ),
        )

    def parts_from(source, r):
        return (
            pltpu.make_async_remote_copy(
                src_ref=o_send.at[me, r],
                dst_ref=o_recv.at[source, r],
                send_sem=o_sems.at[0, source, r],
                recv_sem=o_sems.at[1, source, r],
                device_id={"tensor": partner},
                device_id_type=MESH,
            ),
            pltpu.make_async_remote_copy(
                src_ref=st_send.at[me, r],
                dst_ref=st_recv.at[source, r],
                send_sem=st_sems.at[0, source, r],
                recv_sem=st_sems.at[1, source, r],
                device_id={"tensor": partner},
                device_id_type=MESH,
            ),
        )

    joint = rows % LANES == 0
    pieces = ((0, 2 * rows),) if joint else ((0, rows), (rows, rows))

    def unit(owner_chip, r):
        g = group_of(owner_chip)
        for start, count in pieces:
            q = q_all[owner_chip, r, pl.ds(start, count), :]
            s = lax.dot_general(
                keys[r, g], q, (((1,), (1,)), ((), ())), preferred_element_type=jnp.float32
            )
            slot = me * slots + lax.broadcasted_iota(jnp.int32, (slots, count), 0)
            token = lax.rem(lax.broadcasted_iota(jnp.int32, (1, count), 1), span)
            s = jnp.where(slot <= prefix_ref[r] + token, s, masked_value)
            peak = jnp.maximum(jnp.max(s, axis=0, keepdims=True), lowest_peak)
            p = jnp.exp2((s - peak) * coef)
            total = jnp.sum(p, axis=0, keepdims=True)
            o = lax.dot_general(
                values[r, g],
                p.astype(jnp.bfloat16),
                (((0,), (0,)), ((), ())),
                preferred_element_type=jnp.float32,
            )
            row = lax.broadcasted_iota(jnp.int32, (8, count), 0)
            stats = jnp.where(row < 4, peak, total)
            for k in range(count // rows):
                target = owner_chip * 2 + start // rows + k
                o_send[target, r] = o[:, k * rows : (k + 1) * rows].astype(jnp.bfloat16)
                st_send[target, r] = stats[:, k * rows : (k + 1) * rows]

    def own_unit(r, carry):
        g = group_of(chip)
        kv_copy(0, r, g).wait()
        kv_copy(1, r, g).wait()
        q_piece(chip, 1 - core, r, 0, partner).wait_recv()
        unit(chip, r)
        for copy in parts_to(partner, r):
            copy.start()
        for d in range(1, chips):
            q_piece(other_chip(d), core, r, 0, partner).wait_recv()
            q_piece(other_chip(d), core, r, chips - 1 + d, partner).start()
        return carry

    lax.fori_loop(0, requests, own_unit, 0)

    for gi in range(1, n_groups):
        for r in range(requests):
            g = lax.rem(group_of(chip) + gi, n_groups)
            kv_copy(0, r, g).wait()
            kv_copy(1, r, g).wait()

    def far_unit(i, carry):
        c = other_chip(1 + i // requests)
        r = lax.rem(i, requests)
        q_piece(c, 1 - core, r, 0, partner).wait_recv()
        unit(c, r)
        for k in range(2):
            for copy in parts_to(c * 2 + k, r):
                copy.start()
        return carry

    lax.fori_loop(0, (chips - 1) * requests, far_unit, 0)

    w_copy.wait()
    lane_blocks = width // LANES
    per_depth = lane_blocks * col_groups
    block = 16 * per_depth
    to_row = lax.broadcasted_iota(jnp.int32, (block, block), 0)
    from_row = lax.broadcasted_iota(jnp.int32, (block, block), 1)
    order = jnp.where(
        from_row == lax.rem(to_row, 16) * per_depth + to_row // 16, 1.0, 0.0
    ).astype(jnp.bfloat16)

    def reorder(i, carry):
        pair = jnp.concatenate(
            [w_raw[pl.ds((2 * i + k) * block, block), :] for k in range(2)], axis=1
        )
        ordered = jnp.dot(order, pair, preferred_element_type=jnp.float32).astype(jnp.bfloat16)
        for j in range(lane_blocks):
            for g in range(col_groups):
                at = (j * col_groups + g) * 16
                for k in range(2):
                    w_ready[g, pl.ds((2 * i + k) * 16, 16), j * LANES : (j + 1) * LANES] = ordered[
                        at : at + 16, k * LANES : (k + 1) * LANES
                    ]
        return carry

    lax.fori_loop(0, depth // 32, reorder, 0)

    def att_piece(owner, r, hop, target):
        piece = att.at[owner, pl.ds(r * span, span)]
        return pltpu.make_async_remote_copy(
            src_ref=piece,
            dst_ref=piece,
            send_sem=att_send_sem.at[hop, r],
            recv_sem=att_recv_sem.at[owner, r],
            device_id={"tensor": target},
            device_id_type=MESH,
        )

    def join(r, carry):
        sources = [lax.rem(me + i, n_tensor) for i in range(n_tensor)]
        for source in sources[1:]:
            for copy in parts_from(source, r):
                copy.wait_recv()
        stats = [st_send[me, r]] + [st_recv[source, r] for source in sources[1:]]
        peak = functools.reduce(jnp.maximum, [s[0:1] for s in stats])
        factors = [jnp.exp2((s[0:1] - peak) * coef) for s in stats]
        total = sum(s[4:5] * f for s, f in zip(stats, factors))
        summed = o_send[me, r].astype(jnp.float32) * factors[0]
        for source, factor in zip(sources[1:], factors[1:]):
            summed = summed + o_recv[source, r].astype(jnp.float32) * factor
        done = (summed / total).T.astype(jnp.bfloat16)
        for h in range(heads):
            att[me, pl.ds(r * span, span), h * HD : (h + 1) * HD] = done[h * span : (h + 1) * span]
        for d in range(1, chips):
            att_piece(me, r, d, other_chip(d) * 2 + core).start()
        att_piece(me, r, 0, partner).start()
        return carry

    lax.fori_loop(0, requests, join, 0)

    def term(owner, g):
        return jnp.dot(
            att[owner],
            w_ready[g, pl.ds(owner * depth_each, depth_each), :],
            preferred_element_type=jnp.float32,
        )

    def own_term(g, carry):
        acc[g] = term(me, g)
        return carry

    lax.fori_loop(0, col_groups, own_term, 0)

    def relay(r, carry):
        for d in range(1, chips):
            owner = other_chip(d) * 2 + core
            att_piece(owner, r, 0, partner).wait_recv()
            att_piece(owner, r, chips - 1 + d, partner).start()
        return carry

    lax.fori_loop(0, requests, relay, 0)

    def partner_arrives(r, carry):
        att_piece(partner, r, 0, partner).wait_recv()
        return carry

    lax.fori_loop(0, requests, partner_arrives, 0)

    near = [partner] + [other_chip(d) * 2 + core for d in range(1, chips)]

    def near_terms(g, carry):
        acc[g] += sum(term(owner, g) for owner in near)
        return carry

    lax.fori_loop(0, col_groups, near_terms, 0)

    last = [other_chip(d) * 2 + 1 - core for d in range(1, chips)]

    def last_arrives(r, carry):
        for owner in last:
            att_piece(owner, r, 0, partner).wait_recv()
        return carry

    lax.fori_loop(0, requests, last_arrives, 0)

    def share_to(target):
        return pltpu.make_async_remote_copy(
            src_ref=p_send.at[target],
            dst_ref=p_recv.at[me_p],
            send_sem=p_sems.at[0, target],
            recv_sem=p_sems.at[1, me_p],
            device_id={"pipe": target},
            device_id_type=MESH,
        )

    def share_from(source):
        return pltpu.make_async_remote_copy(
            src_ref=p_send.at[source],
            dst_ref=p_recv.at[source],
            send_sem=p_sems.at[0, source],
            recv_sem=p_sems.at[1, source],
            device_id={"pipe": source},
            device_id_type=MESH,
        )

    def finish_share(g):
        p_send[g] = (acc[g] + sum(term(owner, g) for owner in last)).astype(jnp.bfloat16)

    def send_share(i, carry):
        g = lax.rem(me_p + 1 + lax.rem(i + 1, n_pipe - 1), n_pipe)
        finish_share(g)
        share_to(g).start()
        return carry

    lax.fori_loop(0, n_pipe - 1, send_share, 0)
    finish_share(me_p)

    updated = res_ref[...].astype(jnp.float32) + p_send[me_p].astype(jnp.float32)
    for i in (1, 3, 2) if n_pipe == 4 else range(1, n_pipe):
        source = lax.rem(me_p + i, n_pipe)
        share_from(source).wait_recv()
        updated = updated + p_recv[source].astype(jnp.float32)

    mine = jnp.sum(updated * updated, axis=1, keepdims=True)
    sq_send[...] = jnp.broadcast_to(mine, (tokens, LANES)).T[0:8]

    def squares(other, slot_sem, recv_index, recv_slot):
        return pltpu.make_async_remote_copy(
            src_ref=sq_send,
            dst_ref=sq_recv.at[recv_slot],
            send_sem=sq_sems.at[0, slot_sem],
            recv_sem=sq_sems.at[1, recv_index],
            device_id={"pipe": other // n_tensor, "tensor": lax.rem(other, n_tensor)},
            device_id_type=MESH,
        )

    def send_squares(i, carry):
        other = lax.rem(flat + i, devices)
        squares(other, other, flat, flat).start()
        return carry

    lax.fori_loop(1, devices, send_squares, 0)
    residual_out[...] = updated.astype(residual_out.dtype)
    scaled = updated * gain_ref[...]

    def take_squares(i, so_far):
        other = lax.rem(flat + i, devices)
        squares(other, other, other, other).wait_recv()
        return so_far + sq_recv[other]

    all_squares = lax.fori_loop(1, devices, take_squares, sq_send[...])
    mean = all_squares[0:1] / (devices * width)
    factor = jnp.broadcast_to(lax.rsqrt(mean + epsilon), (LANES, tokens)).T[:, 0:1]
    normed_out[...] = (scaled * factor).astype(normed_out.dtype)

    def end_squares(i, carry):
        other = lax.rem(flat + i, devices)
        squares(other, other, other, other).wait_send()
        return carry

    lax.fori_loop(1, devices, end_squares, 0)
    for i in range(1, n_pipe):
        share_to(lax.rem(me_p + i, n_pipe)).wait_send()

    def end_pieces(r, carry):
        for hop in range(2 * chips - 1):
            q_piece(chip, core, r, hop, partner).wait_send()
            att_piece(me, r, hop, partner).wait_send()
        for i in range(1, n_tensor):
            for copy in parts_to(lax.rem(me + i, n_tensor), r):
                copy.wait_send()
        return carry

    lax.fori_loop(0, requests, end_pieces, 0)


def on_device(
    n_pipe,
    n_tensor,
    queries,
    cache_keys,
    cache_values,
    prefix_lengths,
    residual_in,
    out_weight,
    norm_gain,
):
    tokens, columns = queries.shape
    requests, slots, kv_columns = cache_keys.shape
    groups = kv_columns // HD
    depth, col_groups, width = out_weight.shape
    span = tokens // requests
    rows = columns // HD * span
    chips = n_tensor // 2
    blocks = width // LANES
    w = (
        out_weight.reshape(depth, col_groups, blocks, LANES)
        .transpose(0, 2, 1, 3)
        .reshape(depth * blocks * col_groups, LANES)
    )
    bf16, f32 = jnp.bfloat16, jnp.float32
    dma = pltpu.SemaphoreType.DMA
    vmem = pl.BlockSpec(memory_space=pltpu.VMEM)
    hbm = pl.BlockSpec(memory_space=pl.ANY)
    hops = 2 * chips - 1
    out = jax.ShapeDtypeStruct((tokens, width), bf16)
    return pl.pallas_call(
        functools.partial(kernel, n_pipe, n_tensor, requests),
        out_shape=(out, out),
        in_specs=[pl.BlockSpec(memory_space=pltpu.SMEM), hbm, hbm, hbm, hbm, vmem, vmem],
        out_specs=(vmem, vmem),
        scratch_shapes=[
            pltpu.VMEM((chips, requests, 2 * rows, HD), bf16),
            pltpu.VMEM((requests, groups, slots, HD), bf16),
            pltpu.VMEM((requests, groups, slots, HD), bf16),
            pltpu.VMEM(w.shape, bf16),
            pltpu.VMEM((col_groups, depth, width), bf16),
            pltpu.VMEM((n_tensor, requests, HD, rows), bf16),
            pltpu.VMEM((n_tensor, requests, 8, rows), f32),
            pltpu.VMEM((n_tensor, requests, HD, rows), bf16),
            pltpu.VMEM((n_tensor, requests, 8, rows), f32),
            pltpu.VMEM((n_tensor, tokens, columns), bf16),
            pltpu.VMEM((col_groups, tokens, width), f32),
            pltpu.VMEM((n_pipe, tokens, width), bf16),
            pltpu.VMEM((n_pipe, tokens, width), bf16),
            pltpu.VMEM((8, tokens), f32),
            pltpu.VMEM((n_pipe * n_tensor, 8, tokens), f32),
            dma((requests, columns // HD)),
            dma((2, requests, groups)),
            dma,
            dma((hops, requests)),
            dma((n_tensor, requests)),
            dma((2, n_tensor, requests)),
            dma((2, n_tensor, requests)),
            dma((hops, requests)),
            dma((n_tensor, requests)),
            dma((2, n_pipe)),
            dma((2, n_pipe * n_tensor)),
        ],
        compiler_params=pltpu.CompilerParams(
            collective_id=0, has_side_effects=True, vmem_limit_bytes=60 * 1024 * 1024
        ),
    )(
        prefix_lengths,
        queries,
        cache_keys,
        cache_values,
        w,
        residual_in,
        norm_gain.reshape(1, width),
    )


def solution(mesh):
    in_specs = (
        P("replica", ("pipe", "tensor")),
        P("replica", "tensor", "pipe"),
        P("replica", "tensor", "pipe"),
        P("replica"),
        P("replica", ("pipe", "tensor")),
        P("pipe", None, "tensor"),
        P(("pipe", "tensor")),
    )
    out_specs = (P("replica", ("pipe", "tensor")), P("replica", ("pipe", "tensor")))
    return jax.shard_map(
        functools.partial(on_device, mesh.shape["pipe"], mesh.shape["tensor"]),
        mesh=mesh,
        in_specs=in_specs,
        out_specs=out_specs,
        check_vma=False,
    )
```

```python
import functools
import math

import jax
import jax.numpy as jnp
from jax import lax
from jax.experimental import pallas as pl
from jax.experimental.pallas import tpu as pltpu
from jax.sharding import PartitionSpec as P

HD = 128
LANES = 128
masked_value = -1e30
lowest_peak = -1e29
epsilon = 1e-05
MESH = pl.DeviceIdType.MESH


def kernel(
    n_pipe,
    n_tensor,
    requests,
    prefix_ref,
    q_hbm,
    k_hbm,
    v_hbm,
    w_hbm,
    res_ref,
    gain_ref,
    residual_out,
    normed_out,
    q_all,
    keys,
    values,
    w_raw,
    w_ready,
    o_send,
    st_send,
    o_recv,
    st_recv,
    att,
    acc,
    p_send,
    p_recv,
    sq_send,
    sq_recv,
    q_local_sem,
    kv_sem,
    w_sem,
    q_send_sem,
    q_recv_sem,
    o_sems,
    st_sems,
    att_send_sem,
    att_recv_sem,
    p_sems,
    sq_sems,
):
    tokens = res_ref.shape[0]
    span = tokens // requests
    heads = q_hbm.shape[1] // HD
    rows = heads * span
    chips = n_tensor // 2
    n_groups, slots = keys.shape[1], keys.shape[2]
    group_size = n_tensor * heads // n_groups
    col_groups, depth, width = w_ready.shape
    depth_each = depth // n_tensor
    devices = n_pipe * n_tensor
    coef = math.log2(math.e) / math.sqrt(HD)

    me_p = lax.axis_index("pipe")
    me = lax.axis_index("tensor")
    chip = me // 2
    core = lax.rem(me, 2)
    partner = chip * 2 + 1 - core
    flat = me_p * n_tensor + me

    def other_chip(d):
        return lax.rem(chip + d, chips)

    def group_of(c):
        return (c * 2 * heads) // group_size

    def q_local(r, h):
        return pltpu.make_async_copy(
            q_hbm.at[pl.ds(r * span, span), pl.ds(h * HD, HD)],
            q_all.at[chip, r, pl.ds(core * rows + h * span, span)],
            q_local_sem.at[r, h],
        )

    def kv_copy(which, r, g):
        src, dst = ((k_hbm, keys), (v_hbm, values))[which]
        return pltpu.make_async_copy(
            src.at[r, :, pl.ds(pl.multiple_of(g * HD, HD), HD)], dst.at[r, g], kv_sem.at[which, r, g]
        )

    for r in range(requests):
        for h in range(heads):
            q_local(r, h).start()
    for gi in range(n_groups):
        for r in range(requests):
            g = lax.rem(group_of(chip) + gi, n_groups)
            kv_copy(0, r, g).start()
            kv_copy(1, r, g).start()
    w_copy = pltpu.make_async_copy(w_hbm, w_raw, w_sem)
    w_copy.start()

    barrier = pltpu.get_barrier_semaphore()

    def greet(i, carry):
        other = lax.rem(flat + i, devices)
        pl.semaphore_signal(
            barrier,
            inc=1,
            device_id={"pipe": other // n_tensor, "tensor": lax.rem(other, n_tensor)},
            device_id_type=MESH,
        )
        return carry

    lax.fori_loop(1, devices, greet, 0)
    pl.semaphore_wait(barrier, devices - 1)

    def q_piece(owner_chip, owner_core, r, hop, target):
        piece = q_all.at[owner_chip, r, pl.ds(owner_core * rows, rows)]
        return pltpu.make_async_remote_copy(
            src_ref=piece,
            dst_ref=piece,
            send_sem=q_send_sem.at[hop, r],
            recv_sem=q_recv_sem.at[owner_chip * 2 + owner_core, r],
            device_id={"tensor": target},
            device_id_type=MESH,
        )

    for r in range(requests):
        for h in range(heads):
            q_local(r, h).wait()
        for d in range(1, chips):
            q_piece(chip, core, r, d, other_chip(d) * 2 + core).start()
        q_piece(chip, core, r, 0, partner).start()

    def parts_to(target, r):
        return (
            pltpu.make_async_remote_copy(
                src_ref=o_send.at[target, r],
                dst_ref=o_recv.at[me, r],
                send_sem=o_sems.at[0, target, r],
                recv_sem=o_sems.at[1, me, r],
                device_id={"tensor": target},
                device_id_type=MESH,
            ),
            pltpu.make_async_remote_copy(
                src_ref=st_send.at[target, r],
                dst_ref=st_recv.at[me, r],
                send_sem=st_sems.at[0, target, r],
                recv_sem=st_sems.at[1, me, r],
                device_id={"tensor": target},
                device_id_type=MESH,
            ),
        )

    def parts_from(source, r):
        return (
            pltpu.make_async_remote_copy(
                src_ref=o_send.at[me, r],
                dst_ref=o_recv.at[source, r],
                send_sem=o_sems.at[0, source, r],
                recv_sem=o_sems.at[1, source, r],
                device_id={"tensor": partner},
                device_id_type=MESH,
            ),
            pltpu.make_async_remote_copy(
                src_ref=st_send.at[me, r],
                dst_ref=st_recv.at[source, r],
                send_sem=st_sems.at[0, source, r],
                recv_sem=st_sems.at[1, source, r],
                device_id={"tensor": partner},
                device_id_type=MESH,
            ),
        )

    joint = rows % LANES == 0
    pieces = ((0, 2 * rows),) if joint else ((0, rows), (rows, rows))

    def unit(owner_chip, r):
        g = group_of(owner_chip)
        for start, count in pieces:
            q = q_all[owner_chip, r, pl.ds(start, count), :]
            s = lax.dot_general(
                keys[r, g], q, (((1,), (1,)), ((), ())), preferred_element_type=jnp.float32
            )
            slot = me * slots + lax.broadcasted_iota(jnp.int32, (slots, count), 0)
            token = lax.rem(lax.broadcasted_iota(jnp.int32, (1, count), 1), span)
            s = jnp.where(slot <= prefix_ref[r] + token, s, masked_value)
            peak = jnp.maximum(jnp.max(s, axis=0, keepdims=True), lowest_peak)
            p = jnp.exp2((s - peak) * coef)
            total = jnp.sum(p, axis=0, keepdims=True)
            o = lax.dot_general(
                values[r, g],
                p.astype(jnp.bfloat16),
                (((0,), (0,)), ((), ())),
                preferred_element_type=jnp.float32,
            )
            row = lax.broadcasted_iota(jnp.int32, (8, count), 0)
            stats = jnp.where(row < 4, peak, total)
            for k in range(count // rows):
                target = owner_chip * 2 + start // rows + k
                o_send[target, r] = o[:, k * rows : (k + 1) * rows].astype(jnp.bfloat16)
                st_send[target, r] = stats[:, k * rows : (k + 1) * rows]

    def own_unit(r, carry):
        g = group_of(chip)
        kv_copy(0, r, g).wait()
        kv_copy(1, r, g).wait()
        q_piece(chip, 1 - core, r, 0, partner).wait_recv()
        unit(chip, r)
        for copy in parts_to(partner, r):
            copy.start()
        for d in range(1, chips):
            q_piece(other_chip(d), core, r, 0, partner).wait_recv()
            q_piece(other_chip(d), core, r, chips - 1 + d, partner).start()
        return carry

    lane_blocks = width // LANES
    per_depth = lane_blocks * col_groups
    block = 16 * per_depth
    wide = 4
    to_row = lax.broadcasted_iota(jnp.int32, (block, block), 0)
    from_row = lax.broadcasted_iota(jnp.int32, (block, block), 1)
    order = jnp.where(
        from_row == lax.rem(to_row, 16) * per_depth + to_row // 16, 1.0, 0.0
    ).astype(jnp.bfloat16)

    def reorder(i, carry):
        pair = jnp.concatenate(
            [w_raw[pl.ds((wide * i + k) * block, block), :] for k in range(wide)], axis=1
        )
        ordered = jnp.dot(order, pair, preferred_element_type=jnp.float32).astype(jnp.bfloat16)
        for j in range(lane_blocks):
            for g in range(col_groups):
                at = (j * col_groups + g) * 16
                for k in range(wide):
                    w_ready[g, pl.ds((wide * i + k) * 16, 16), j * LANES : (j + 1) * LANES] = ordered[
                        at : at + 16, k * LANES : (k + 1) * LANES
                    ]
        return carry

    def reorder_of(owner):
        steps = depth_each // (16 * wide)
        lax.fori_loop(owner * steps, (owner + 1) * steps, reorder, 0)

    w_copy.wait()
    reorder_of(me)

    lax.fori_loop(0, requests, own_unit, 0)

    for gi in range(1, n_groups):
        for r in range(requests):
            g = lax.rem(group_of(chip) + gi, n_groups)
            kv_copy(0, r, g).wait()
            kv_copy(1, r, g).wait()

    def far_unit(i, carry):
        c = other_chip(1 + i // requests)
        r = lax.rem(i, requests)
        q_piece(c, 1 - core, r, 0, partner).wait_recv()
        unit(c, r)
        for k in range(2):
            for copy in parts_to(c * 2 + k, r):
                copy.start()
        return carry

    lax.fori_loop(0, (chips - 1) * requests, far_unit, 0)

    near = [partner] + [other_chip(d) * 2 + core for d in range(1, chips)]
    last = [other_chip(d) * 2 + 1 - core for d in range(1, chips)]
    for owner in near:
        reorder_of(owner)

    def att_piece(owner, r, hop, target):
        piece = att.at[owner, pl.ds(r * span, span)]
        return pltpu.make_async_remote_copy(
            src_ref=piece,
            dst_ref=piece,
            send_sem=att_send_sem.at[hop, r],
            recv_sem=att_recv_sem.at[owner, r],
            device_id={"tensor": target},
            device_id_type=MESH,
        )

    def join(r, carry):
        sources = [lax.rem(me + i, n_tensor) for i in range(n_tensor)]
        for source in sources[1:]:
            for copy in parts_from(source, r):
                copy.wait_recv()
        stats = [st_send[me, r]] + [st_recv[source, r] for source in sources[1:]]
        peak = functools.reduce(jnp.maximum, [s[0:1] for s in stats])
        factors = [jnp.exp2((s[0:1] - peak) * coef) for s in stats]
        total = sum(s[4:5] * f for s, f in zip(stats, factors))
        summed = o_send[me, r].astype(jnp.float32) * factors[0]
        for source, factor in zip(sources[1:], factors[1:]):
            summed = summed + o_recv[source, r].astype(jnp.float32) * factor
        done = (summed / total).T.astype(jnp.bfloat16)
        for h in range(heads):
            att[me, pl.ds(r * span, span), h * HD : (h + 1) * HD] = done[h * span : (h + 1) * span]
        for d in range(1, chips):
            att_piece(me, r, d, other_chip(d) * 2 + core).start()
        att_piece(me, r, 0, partner).start()
        return carry

    lax.fori_loop(0, requests, join, 0)

    def term(owner, g):
        return jnp.dot(
            att[owner],
            w_ready[g, pl.ds(owner * depth_each, depth_each), :],
            preferred_element_type=jnp.float32,
        )

    def own_term(g, carry):
        acc[g] = term(me, g)
        return carry

    lax.fori_loop(0, col_groups, own_term, 0)
    for owner in last:
        reorder_of(owner)

    def relay(r, carry):
        for d in range(1, chips):
            owner = other_chip(d) * 2 + core
            att_piece(owner, r, 0, partner).wait_recv()
            att_piece(owner, r, chips - 1 + d, partner).start()
        return carry

    lax.fori_loop(0, requests, relay, 0)

    def partner_arrives(r, carry):
        att_piece(partner, r, 0, partner).wait_recv()
        return carry

    lax.fori_loop(0, requests, partner_arrives, 0)

    def near_terms(g, carry):
        acc[g] += sum(term(owner, g) for owner in near)
        return carry

    lax.fori_loop(0, col_groups, near_terms, 0)

    def last_arrives(r, carry):
        for owner in last:
            att_piece(owner, r, 0, partner).wait_recv()
        return carry

    lax.fori_loop(0, requests, last_arrives, 0)

    def share_to(target):
        return pltpu.make_async_remote_copy(
            src_ref=p_send.at[target],
            dst_ref=p_recv.at[me_p],
            send_sem=p_sems.at[0, target],
            recv_sem=p_sems.at[1, me_p],
            device_id={"pipe": target},
            device_id_type=MESH,
        )

    def share_from(source):
        return pltpu.make_async_remote_copy(
            src_ref=p_send.at[source],
            dst_ref=p_recv.at[source],
            send_sem=p_sems.at[0, source],
            recv_sem=p_sems.at[1, source],
            device_id={"pipe": source},
            device_id_type=MESH,
        )

    def finish_share(g):
        p_send[g] = (acc[g] + sum(term(owner, g) for owner in last)).astype(jnp.bfloat16)

    def send_share(i, carry):
        g = lax.rem(me_p + 1 + lax.rem(i + 1, n_pipe - 1), n_pipe)
        finish_share(g)
        share_to(g).start()
        return carry

    lax.fori_loop(0, n_pipe - 1, send_share, 0)
    finish_share(me_p)

    updated = res_ref[...].astype(jnp.float32) + p_send[me_p].astype(jnp.float32)
    for i in (1, 3, 2) if n_pipe == 4 else range(1, n_pipe):
        source = lax.rem(me_p + i, n_pipe)
        share_from(source).wait_recv()
        updated = updated + p_recv[source].astype(jnp.float32)

    mine = jnp.sum(updated * updated, axis=1, keepdims=True)
    sq_send[...] = jnp.broadcast_to(mine, (tokens, LANES)).T[0:1]

    def squares(other, slot_sem, recv_index, recv_slot):
        return pltpu.make_async_remote_copy(
            src_ref=sq_send,
            dst_ref=sq_recv.at[recv_slot],
            send_sem=sq_sems.at[0, slot_sem],
            recv_sem=sq_sems.at[1, recv_index],
            device_id={"pipe": other // n_tensor, "tensor": lax.rem(other, n_tensor)},
            device_id_type=MESH,
        )

    def send_squares(i, carry):
        other = lax.rem(flat + i, devices)
        squares(other, other, flat, flat).start()
        return carry

    lax.fori_loop(1, devices, send_squares, 0)
    residual_out[...] = updated.astype(residual_out.dtype)
    scaled = updated * gain_ref[...]

    def take_squares(i, so_far):
        other = lax.rem(flat + i, devices)
        squares(other, other, other, other).wait_recv()
        return so_far + sq_recv[other]

    all_squares = lax.fori_loop(1, devices, take_squares, sq_send[...])
    mean = all_squares / (devices * width)
    factor = jnp.broadcast_to(lax.rsqrt(mean + epsilon), (LANES, tokens)).T[:, 0:1]
    normed_out[...] = (scaled * factor).astype(normed_out.dtype)

    def end_squares(i, carry):
        other = lax.rem(flat + i, devices)
        squares(other, other, other, other).wait_send()
        return carry

    lax.fori_loop(1, devices, end_squares, 0)
    for i in range(1, n_pipe):
        share_to(lax.rem(me_p + i, n_pipe)).wait_send()

    def end_pieces(r, carry):
        for hop in range(2 * chips - 1):
            q_piece(chip, core, r, hop, partner).wait_send()
            att_piece(me, r, hop, partner).wait_send()
        for i in range(1, n_tensor):
            for copy in parts_to(lax.rem(me + i, n_tensor), r):
                copy.wait_send()
        return carry

    lax.fori_loop(0, requests, end_pieces, 0)


def on_device(
    n_pipe,
    n_tensor,
    queries,
    cache_keys,
    cache_values,
    prefix_lengths,
    residual_in,
    out_weight,
    norm_gain,
):
    tokens, columns = queries.shape
    requests, slots, kv_columns = cache_keys.shape
    groups = kv_columns // HD
    depth, col_groups, width = out_weight.shape
    span = tokens // requests
    rows = columns // HD * span
    chips = n_tensor // 2
    blocks = width // LANES
    w = (
        out_weight.reshape(depth, col_groups, blocks, LANES)
        .transpose(0, 2, 1, 3)
        .reshape(depth * blocks * col_groups, LANES)
    )
    bf16, f32 = jnp.bfloat16, jnp.float32
    dma = pltpu.SemaphoreType.DMA
    vmem = pl.BlockSpec(memory_space=pltpu.VMEM)
    hbm = pl.BlockSpec(memory_space=pl.ANY)
    hops = 2 * chips - 1
    out = jax.ShapeDtypeStruct((tokens, width), bf16)
    return pl.pallas_call(
        functools.partial(kernel, n_pipe, n_tensor, requests),
        out_shape=(out, out),
        in_specs=[pl.BlockSpec(memory_space=pltpu.SMEM), hbm, hbm, hbm, hbm, vmem, vmem],
        out_specs=(vmem, vmem),
        scratch_shapes=[
            pltpu.VMEM((chips, requests, 2 * rows, HD), bf16),
            pltpu.VMEM((requests, groups, slots, HD), bf16),
            pltpu.VMEM((requests, groups, slots, HD), bf16),
            pltpu.VMEM(w.shape, bf16),
            pltpu.VMEM((col_groups, depth, width), bf16),
            pltpu.VMEM((n_tensor, requests, HD, rows), bf16),
            pltpu.VMEM((n_tensor, requests, 8, rows), f32),
            pltpu.VMEM((n_tensor, requests, HD, rows), bf16),
            pltpu.VMEM((n_tensor, requests, 8, rows), f32),
            pltpu.VMEM((n_tensor, tokens, columns), bf16),
            pltpu.VMEM((col_groups, tokens, width), f32),
            pltpu.VMEM((n_pipe, tokens, width), bf16),
            pltpu.VMEM((n_pipe, tokens, width), bf16),
            pltpu.VMEM((1, tokens), f32),
            pltpu.VMEM((n_pipe * n_tensor, 1, tokens), f32),
            dma((requests, columns // HD)),
            dma((2, requests, groups)),
            dma,
            dma((hops, requests)),
            dma((n_tensor, requests)),
            dma((2, n_tensor, requests)),
            dma((2, n_tensor, requests)),
            dma((hops, requests)),
            dma((n_tensor, requests)),
            dma((2, n_pipe)),
            dma((2, n_pipe * n_tensor)),
        ],
        compiler_params=pltpu.CompilerParams(
            collective_id=0, has_side_effects=True, vmem_limit_bytes=60 * 1024 * 1024
        ),
    )(
        prefix_lengths,
        queries,
        cache_keys,
        cache_values,
        w,
        residual_in,
        norm_gain.reshape(1, width),
    )


def solution(mesh):
    in_specs = (
        P("replica", ("pipe", "tensor")),
        P("replica", "tensor", "pipe"),
        P("replica", "tensor", "pipe"),
        P("replica"),
        P("replica", ("pipe", "tensor")),
        P("pipe", None, "tensor"),
        P(("pipe", "tensor")),
    )
    out_specs = (P("replica", ("pipe", "tensor")), P("replica", ("pipe", "tensor")))
    return jax.shard_map(
        functools.partial(on_device, mesh.shape["pipe"], mesh.shape["tensor"]),
        mesh=mesh,
        in_specs=in_specs,
        out_specs=out_specs,
        check_vma=False,
    )
```
